32 devices in a mesh: section: 4 (over y, x), tp: 8 (over z, core).
Axes of the slice: x: 2, y: 2, z: 4, core: 2. Of those that a mesh axis runs over, the one named last changes fastest.
Arguments:
- grad_in: bfloat16 [4, 128, 4096], P('section', None, 'tp'), may hold values from -6 to 6
- fresh_grads: bfloat16 [1, 128, 4096], P(None, None, 'tp'), may hold values from -6 to 6
- acc_in: float32 [4, 128, 4096], P('section', None, 'tp'), may hold values from -3 to 3
- queries: bfloat16 [4, 2, 128, 4096], P('section', None, None, 'tp'), may hold values from -4.625 to 4.625
- keys: bfloat16 [4, 2, 128, 4096], P('section', None, None, 'tp'), may hold values from -4.625 to 4.625
- values: bfloat16 [4, 2, 128, 4096], P('section', None, None, 'tp'), may hold values from -12 to 12
- query_weight: bfloat16 [4, 4096, 4096], P('section', 'tp'), may hold values from -0.09375 to 0.09375
- key_weight: bfloat16 [4, 4096, 4096], P('section', None, 'tp'), may hold values from -0.125 to 0.125
- value_weight: bfloat16 [4, 4096, 4096], P('section', None, 'tp'), may hold values from -0.125 to 0.125
- out_weight: bfloat16 [4, 4096, 4096], P('section', 'tp'), may hold values from -0.09375 to 0.09375
Outputs:
- grad_out: bfloat16 [4, 128, 4096], P('section', None, 'tp')
- acc_out: float32 [4, 128, 4096], P('section', None, 'tp')
The draws below stay inside these ranges and needn't reach their ends.
All inputs are finite; a program needn't handle non-finite values.
Results may differ from the reference program's by a relative error of at most 0.025.
Values may be sent and summed in bfloat16 or wider, within the bound.
A program may use at most 64 MiB of HBM per device.

```python
import jax
import jax.numpy as jnp
from jax import lax

D = 4096
HEADS = 64
HEAD_DIM = 64
SEQS = 1
DEC_LEN = 128
ENC_LEN = 128
MICRO = 2
SECTIONS = 4
INNER = 4096
TOK = 128
ENC_ROWS = 128
N_TP = 8


def draw_queries(key, part):
    noise_key = jax.random.fold_in(key, 1)
    full_shape = (SECTIONS, MICRO, SEQS, DEC_LEN, HEADS, HEAD_DIM)
    field = jnp.clip(0.35 * jax.random.normal(noise_key, full_shape, jnp.float32), -2.5, 2.5)
    return field.reshape(SECTIONS, MICRO, SEQS * DEC_LEN, HEADS * HEAD_DIM).astype(jnp.bfloat16)


def draw_keys(key, part):
    noise_key = jax.random.fold_in(key, 2)
    full_shape = (SECTIONS, MICRO, SEQS, ENC_LEN, HEADS, HEAD_DIM)
    field = jnp.clip(0.5 * jax.random.normal(noise_key, full_shape, jnp.float32), -2.5, 2.5)
    return field.reshape(SECTIONS, MICRO, SEQS * ENC_LEN, HEADS * HEAD_DIM).astype(jnp.bfloat16)


def raised(entries, rng, source, target, parts, factor):
    owner, partner = [(jnp.arange(entries.shape[dim]) // (entries.shape[dim] // parts)).reshape([-1 if axis == dim else 1 for axis in range(entries.ndim)]) for dim in (source, target)]
    chosen = jax.random.permutation(rng, parts)[partner]
    strong = (owner == chosen) | (owner == (partner + parts // 2) % parts)
    return jnp.where(strong, factor * entries, entries)


def block_scale(own_key, dims, cuts, least, largest):
    def one(position, shards_of):
        steps = jax.random.uniform(jax.random.fold_in(jax.random.fold_in(own_key, 6), position), (shards_of,), jnp.float32, least / len(cuts), largest / len(cuts))
        return jnp.repeat(jnp.exp(steps), dims[position] // shards_of).reshape((-1,) + (1,) * (len(dims) - position - 1))

    loudness = one(*cuts[0])
    for cut in cuts[1:]:
        loudness = loudness * one(*cut)
    return loudness


def centred(rng, dims, spread, reach, pieces=(), held_as=jnp.bfloat16):
    result = spread * jax.random.normal(rng, dims, jnp.float32)
    if pieces:
        result = result * block_scale(rng, dims, pieces, -0.22, 0.18)
    return jnp.clip(result, -reach, reach).astype(held_as)


def noise_with(key, shape, deviation, most, pieces, heavy, kind=jnp.bfloat16):
    values = deviation * jax.random.normal(key, shape, jnp.float32)
    if pieces:
        values = values * block_scale(key, shape, pieces, -0.22, 0.18)
    return jnp.clip(raised(values, jax.random.fold_in(key, 3), *heavy), -most, most).astype(kind)


def setup_inputs(seed: int = 0) -> dict:
    splits = jax.random.split(jax.random.key(seed), 11)
    return {
        "grad_in": centred(splits[0], (SECTIONS, TOK, D), 1.0, 6.0, ((0, 4), (2, 8))),
        "fresh_grads": centred(splits[1], (MICRO - 1, TOK, D), 1.0, 6.0, ((2, 8),)),
        "acc_in": centred(splits[2], (SECTIONS, ENC_ROWS, D), 0.5, 3.0, ((0, 4), (2, 8)), jnp.float32),
        "queries": draw_queries(jax.random.fold_in(splits[10], 71), 0),
        "keys": draw_keys(jax.random.fold_in(splits[10], 71), 0),
        "values": centred(splits[5], (SECTIONS, MICRO, ENC_ROWS, INNER), 2.0, 12.0, ((0, 4), (3, 8))),
        "query_weight": centred(splits[6], (SECTIONS, D, INNER), D ** -0.5, 0.09375, ((0, 4), (1, 8))),
        "key_weight": noise_with(splits[7], (SECTIONS, D, INNER), D ** -0.5, 0.125, ((0, 4), (2, 8)), (2, 1, 8, 2.0)),
        "value_weight": noise_with(splits[8], (SECTIONS, D, INNER), D ** -0.5, 0.125, ((0, 4), (2, 8)), (2, 1, 8, 2.0)),
        "out_weight": centred(splits[9], (SECTIONS, INNER, D), INNER ** -0.5, 0.09375, ((0, 4), (1, 8))),
    }


def attention_grads(upstream, queries, keys, values):
    token_rows, columns = queries.shape
    enc_rows = keys.shape[0]
    query_heads = queries.astype(jnp.float32).reshape(SEQS, token_rows // SEQS, HEADS, HEAD_DIM)
    key_heads = keys.astype(jnp.float32).reshape(SEQS, enc_rows // SEQS, HEADS, HEAD_DIM)
    value_heads = values.astype(jnp.float32).reshape(SEQS, enc_rows // SEQS, HEADS, HEAD_DIM)
    upstream_heads = upstream.astype(jnp.float32).reshape(SEQS, token_rows // SEQS, HEADS, HEAD_DIM)
    scores = jnp.einsum("bqhd,bkhd->bhqk", query_heads, key_heads, precision=lax.Precision.HIGHEST)
    attention = jax.nn.softmax(scores, axis=-1)
    weights = attention.astype(jnp.bfloat16).astype(jnp.float32)
    output = jnp.einsum("bhqk,bkhd->bqhd", weights, value_heads, precision=lax.Precision.HIGHEST)
    delta = jnp.sum(upstream_heads * output, axis=-1)
    prob_grad = jnp.einsum("bqhd,bkhd->bhqk", upstream_heads, value_heads, precision=lax.Precision.HIGHEST)
    score_grad = (attention * (prob_grad - jnp.transpose(delta, (0, 2, 1))[..., None])).astype(jnp.bfloat16)
    score_grad = score_grad.astype(jnp.float32)
    query_grad = jnp.einsum("bhqk,bkhd->bqhd", score_grad, key_heads, precision=lax.Precision.HIGHEST)
    key_grad = jnp.einsum("bhqk,bqhd->bkhd", score_grad, query_heads, precision=lax.Precision.HIGHEST)
    value_grad = jnp.einsum("bhqk,bqhd->bkhd", weights, upstream_heads, precision=lax.Precision.HIGHEST)
    return (query_grad.reshape(token_rows, columns).astype(jnp.bfloat16),
            key_grad.reshape(enc_rows, columns).astype(jnp.bfloat16),
            value_grad.reshape(enc_rows, columns).astype(jnp.bfloat16))


def section_step(inputs):
    grad, carried, query_rows, key_rows, value_rows, w_query, w_key, w_value, w_out = inputs
    upstream = jnp.dot(grad, w_out.T, preferred_element_type=jnp.float32).astype(jnp.bfloat16)
    query_grad, key_grad, value_grad = attention_grads(upstream, query_rows, key_rows, value_rows)
    branch = jnp.dot(query_grad, w_query.T, preferred_element_type=jnp.float32)
    passed = (grad.astype(jnp.float32) + branch).astype(jnp.bfloat16)
    group_width = w_key.shape[1] // N_TP
    enc_rows = key_grad.shape[0]
    key_groups = key_grad.astype(jnp.float32).reshape(enc_rows, N_TP, group_width)
    value_groups = value_grad.astype(jnp.float32).reshape(enc_rows, N_TP, group_width)
    key_cols = w_key.astype(jnp.float32).reshape(w_key.shape[0], N_TP, group_width)
    value_cols = w_value.astype(jnp.float32).reshape(w_value.shape[0], N_TP, group_width)
    terms = jnp.einsum("rgc,dgc->grd", key_groups, key_cols, precision=lax.Precision.HIGHEST)
    terms = terms + jnp.einsum("rgc,dgc->grd", value_groups, value_cols, precision=lax.Precision.HIGHEST)
    rounded = lax.optimization_barrier(terms.astype(jnp.bfloat16)).astype(jnp.float32)
    return passed, carried + jnp.sum(rounded, axis=0)


def reference(grad_in, fresh_grads, acc_in, queries, keys, values, query_weight, key_weight, value_weight, out_weight):
    grads = grad_in
    sums = acc_in
    passed = grad_in
    updated = acc_in
    for slot in range(MICRO):
        passed, updated = lax.map(section_step, (grads, sums, queries[:, slot], keys[:, slot], values[:, slot],
                                               query_weight, key_weight, value_weight, out_weight))
        if slot + 1 < MICRO:
            grads = jnp.concatenate([passed[1:], fresh_grads[slot][None]], axis=0)
            sums = jnp.concatenate([updated[1:], jnp.zeros_like(updated[:1])], axis=0)
    return passed, updated
```

```python
import functools

import jax
import jax.numpy as jnp
from jax import lax
from jax.experimental import pallas as pl
from jax.experimental.pallas import tpu as pltpu
from jax.sharding import PartitionSpec as P

HEAD_DIM = 64
LANES = 128
CHUNKS = 2
MESH = pl.DeviceIdType.MESH
F32, BF16 = jnp.float32, jnp.bfloat16


def nt(left, right):
    return lax.dot_general(left, right, (((1,), (1,)), ((), ())), preferred_element_type=F32)


def tn(left, right):
    return lax.dot_general(left, right, (((0,), (0,)), ((), ())), preferred_element_type=F32)


def nn(left, right):
    return lax.dot_general(left, right, (((1,), (0,)), ((), ())), preferred_element_type=F32)


def kernel(
    n_sections, n_tp, slots,
    grad_in, fresh, acc_in, queries, keys, values, wq_hbm, wk_hbm, wv_hbm, wo_hbm,
    grad_out, acc_out,
    wq, wk, wv, wo, gbuf, gathered, qgrad, kgrad, vgrad, total, passed_buf,
    own_term, part_out, part_in, right_out, right_in, left_out, left_in, acc_send, acc_recv,
    load_sem, ag_send, ag_recv, part_sem, right_sem, left_sem, pass_sem, acc_sem,
):
    section = lax.axis_index("section")
    me = lax.axis_index("tp")
    chips = n_tp // 2
    chip, core = me // 2, me % 2
    other = 1 - core
    partner = chip * 2 + other
    rows, width = grad_in.shape[1], grad_in.shape[2]
    columns = queries.shape[3]
    piece = rows // CHUNKS
    has_left, has_right = chip > 0, chip < chips - 1
    top = section == n_sections - 1

    def load(source, target, n):
        return pltpu.make_async_copy(source, target, load_sem.at[n])

    loads = [
        load(grad_in.at[0], gbuf.at[0], 0),
        load(wo_hbm.at[0], wo, 1),
        load(wk_hbm.at[0], wk, 2),
        load(wv_hbm.at[0], wv, 3),
        load(wq_hbm.at[0], wq, 4),
    ]
    for one in loads:
        one.start()

    barrier = pltpu.get_barrier_semaphore()

    def greet(condition, device):
        @pl.when(condition)
        def _():
            pl.semaphore_signal(barrier, inc=1, device_id=device, device_id_type=MESH)

    neighbours = [
        (core >= 0, {"tp": partner}),
        (has_left, {"tp": me - 2}),
        (has_right, {"tp": me + 2}),
        (section > 0, {"section": section - 1}),
        (section < n_sections - 1, {"section": section + 1}),
    ]
    for condition, device in neighbours:
        greet(condition, device)
    pl.semaphore_wait(barrier, sum(jnp.where(condition, 1, 0) for condition, _ in neighbours))

    def part_of(c):
        return pl.ds(c * piece, piece)

    def block_copy(source, i, block, c, way, device):
        return pltpu.make_async_remote_copy(
            src_ref=source.at[part_of(c)],
            dst_ref=gathered.at[i, block, part_of(c)],
            send_sem=ag_send.at[i, block // 2, c, way],
            recv_sem=ag_recv.at[i, block, c],
            device_id={"tp": device},
            device_id_type=MESH,
        )

    def start_gather(i, source):
        for c in range(CHUNKS):
            @pl.when(has_right)
            def _():
                block_copy(source, i, me, c, 0, me + 2).start()

            @pl.when(has_left)
            def _():
                block_copy(source, i, me, c, 1, me - 2).start()

        for c in range(CHUNKS):
            block_copy(source, i, me, c, 2, partner).start()

    def relay(i, h):
        for c in range(CHUNKS):
            @pl.when((h > 0) & (chip - h >= 0))
            def _():
                block = (chip - h) * 2 + core
                held = gathered.at[i, block]
                block_copy(held, i, block, c, 2, partner).wait_recv()

                @pl.when(has_right)
                def _():
                    block_copy(held, i, block, c, 0, me + 2).start()

                block_copy(held, i, block, c, 2, partner).start()

            @pl.when((h > 0) & (chip + h < chips))
            def _():
                block = (chip + h) * 2 + core
                held = gathered.at[i, block]
                block_copy(held, i, block, c, 2, partner).wait_recv()

                @pl.when(has_left)
                def _():
                    block_copy(held, i, block, c, 1, me - 2).start()

                block_copy(held, i, block, c, 2, partner).start()

    def add_block(i, weight, block):
        at = pl.ds(pl.multiple_of(block * (weight.shape[1] // n_tp), LANES), weight.shape[1] // n_tp)
        total[...] += nt(gathered[i, block], weight[:, at])

    def take(i, weight, h):
        for condition, chip_of in (((h > 0) & (chip - h >= 0), chip - h), ((h > 0) & (chip + h < chips), chip + h)):
            @pl.when(condition)
            def _():
                add_block(i, weight, chip_of * 2 + core)

    def take_partner(i, weight, h):
        for condition, chip_of in (((h >= 0) & (chip - h >= 0), chip - h), ((h > 0) & (chip + h < chips), chip + h)):
            @pl.when(condition)
            def _():
                block = chip_of * 2 + other
                for c in range(CHUNKS):
                    block_copy(gathered.at[i, block], i, block, c, 2, partner).wait_recv()
                add_block(i, weight, block)

    def own_block(source, weight):
        at = pl.ds(pl.multiple_of(me * (weight.shape[1] // n_tp), LANES), weight.shape[1] // n_tp)
        total[...] = nt(source[...], weight[:, at])

    def wait_gather_sends(i, source):
        @pl.loop(0, chips)
        def _(o):
            block = o * 2 + core
            for c in range(CHUNKS):
                @pl.when(has_right & (o <= chip))
                def _():
                    block_copy(source, i, block, c, 0, me + 2).wait_send()

                @pl.when(has_left & (o >= chip))
                def _():
                    block_copy(source, i, block, c, 1, me - 2).wait_send()

                block_copy(source, i, block, c, 2, partner).wait_send()

    def attention_grads(slot):
        lane = lax.broadcasted_iota(jnp.int32, (1, LANES), 1)
        masks = [
            ((lane >= n * HEAD_DIM) & (lane < (n + 1) * HEAD_DIM)).astype(F32).astype(BF16)
            for n in range(LANES // HEAD_DIM)
        ]
        for pair in range(columns // LANES):
            at = pl.ds(pair * LANES, LANES)
            query, key, value = queries[0, slot, :, at], keys[0, slot, :, at], values[0, slot, :, at]
            upstream = total[:, at].astype(BF16)
            dq, dk, dv = 0.0, 0.0, 0.0
            for mask in masks:
                key_h = key * mask
                scores = nt(query, key_h)
                prob_grad = nt(upstream, value * mask)
                shifted = jnp.exp(scores - jnp.max(scores, axis=1, keepdims=True))
                attention = shifted / jnp.sum(shifted, axis=1, keepdims=True)
                weights = attention.astype(BF16)
                delta = jnp.sum(weights.astype(F32) * prob_grad, axis=1, keepdims=True)
                score_grad = (attention * (prob_grad - delta)).astype(BF16)
                dq = dq + nn(score_grad, key_h)
                dk = dk + tn(score_grad, query * mask)
                dv = dv + tn(weights, upstream * mask)
            qgrad[slot, :, at] = dq.astype(BF16)
            kgrad[:, at] = dk.astype(BF16)
            vgrad[:, at] = dv.astype(BF16)

    def part_copy(slot, z):
        return pltpu.make_async_remote_copy(
            src_ref=part_out.at[slot, z], dst_ref=part_in.at[slot, z],
            send_sem=part_sem.at[0, slot, z], recv_sem=part_sem.at[1, slot, z],
            device_id={"tp": partner}, device_id_type=MESH,
        )

    def right_copy(slot, z):
        return pltpu.make_async_remote_copy(
            src_ref=right_out.at[slot, z], dst_ref=right_in.at[slot, z],
            send_sem=right_sem.at[0, slot, z], recv_sem=right_sem.at[1, slot, z],
            device_id={"tp": me + 2}, device_id_type=MESH,
        )

    def left_copy(slot, z):
        return pltpu.make_async_remote_copy(
            src_ref=left_out.at[slot, z], dst_ref=left_in.at[slot, z],
            send_sem=left_sem.at[0, slot, z], recv_sem=left_sem.at[1, slot, z],
            device_id={"tp": me - 2}, device_id_type=MESH,
        )

    def term_block(z, core_of):
        at = pl.ds(pl.multiple_of((z * 2 + core_of) * width, LANES), width)
        return nt(kgrad[...], wk[at, :]) + nt(vgrad[...], wv[at, :])

    def make_terms(slot):
        @pl.loop(0, chips)
        def _(z):
            part_out[slot, z] = term_block(z, other).astype(BF16)
            part_copy(slot, z).start()

        @pl.loop(0, chips)
        def _(z):
            own_term[z] = term_block(z, core)

    def sum_step(slot, h):
        @pl.when(chip == h)
        def _():
            @pl.loop(0, chips)
            def _(j):
                z = chips - 1 - j

                @pl.when(z > chip)
                def _():
                    part_copy(slot, z).wait_recv()

                    @pl.when(has_left)
                    def _():
                        right_copy(slot, z).wait_recv()
                        own_term[z] += right_in[slot, z].astype(F32)

                    right_out[slot, z] = (own_term[z] + part_in[slot, z].astype(F32)).astype(BF16)
                    right_copy(slot, z).start()

        @pl.when(chips - 1 - chip == h)
        def _():
            @pl.loop(0, chips)
            def _(z):
                @pl.when(z < chip)
                def _():
                    part_copy(slot, z).wait_recv()

                    @pl.when(has_right)
                    def _():
                        left_copy(slot, z).wait_recv()
                        own_term[z] += left_in[slot, z].astype(F32)

                    left_out[slot, z] = (own_term[z] + part_in[slot, z].astype(F32)).astype(BF16)
                    left_copy(slot, z).start()

    def finish_sum(slot):
        part_copy(slot, chip).wait_recv()
        own_term[chip] += part_in[slot, chip].astype(F32)

        @pl.when(has_left)
        def _():
            right_copy(slot, chip).wait_recv()
            own_term[chip] += right_in[slot, chip].astype(F32)

        @pl.when(has_right)
        def _():
            left_copy(slot, chip).wait_recv()
            own_term[chip] += left_in[slot, chip].astype(F32)

        @pl.when(slot == 0)
        def _():
            own_term[chip] += acc_in[0]

        @pl.when((slot > 0) & (section < n_sections - 1))
        def _():
            acc_copy(slot).wait_recv()
            own_term[chip] += acc_recv[slot].astype(F32)

        @pl.when(slot == slots - 1)
        def _():
            acc_out[0] = own_term[chip]

        @pl.when((slot < slots - 1) & (section > 0))
        def _():
            acc_send[slot] = own_term[chip].astype(BF16)
            acc_copy(slot + 1).start()

    def acc_copy(slot):
        return pltpu.make_async_remote_copy(
            src_ref=acc_send.at[slot - 1], dst_ref=acc_recv.at[slot],
            send_sem=acc_sem.at[0, slot], recv_sem=acc_sem.at[1, slot],
            device_id={"section": section - 1}, device_id_type=MESH,
        )

    def pass_copy(slot):
        return pltpu.make_async_remote_copy(
            src_ref=passed_buf.at[slot - 1], dst_ref=gbuf.at[slot],
            send_sem=pass_sem.at[0, slot], recv_sem=pass_sem.at[1, slot],
            device_id={"section": section - 1}, device_id_type=MESH,
        )

    def fresh_copy(slot):
        return pltpu.make_async_copy(fresh.at[slot - 1], gbuf.at[slot], pass_sem.at[1, slot])

    @pl.loop(0, slots)
    def _(slot):
        @pl.when(slot == 0)
        def _():
            loads[0].wait()

        @pl.when((slot > 0) & top)
        def _():
            fresh_copy(slot).start()
            fresh_copy(slot).wait()

        @pl.when((slot > 0) & (section < n_sections - 1))
        def _():
            pass_copy(slot).wait_recv()

        first = slot * 2
        second = first + 1
        start_gather(first, gbuf.at[slot])

        @pl.when(slot == 0)
        def _():
            loads[1].wait()

        own_block(gbuf.at[slot], wo)

        @pl.loop(1, chips)
        def _(h):
            relay(first, h)
            take(first, wo, h)
            take_partner(first, wo, h - 1)

        take_partner(first, wo, chips - 1)
        attention_grads(slot)
        start_gather(second, qgrad.at[slot])

        @pl.when(slot == 0)
        def _():
            loads[2].wait()
            loads[3].wait()

        make_terms(slot)

        @pl.when(slot == 0)
        def _():
            loads[4].wait()

        own_block(qgrad.at[slot], wq)

        @pl.loop(0, chips)
        def _(h):
            relay(second, h)
            sum_step(slot, h)
            take(second, wq, h)
            take_partner(second, wq, h - 1)

        take_partner(second, wq, chips - 1)
        result = (gbuf[slot].astype(F32) + total[...]).astype(BF16)

        @pl.when(slot == slots - 1)
        def _():
            grad_out[0] = result

        @pl.when((slot < slots - 1) & (section > 0))
        def _():
            passed_buf[slot] = result
            pass_copy(slot + 1).start()

        finish_sum(slot)

    @pl.loop(0, slots)
    def _(slot):
        wait_gather_sends(slot * 2, gbuf.at[slot])
        wait_gather_sends(slot * 2 + 1, qgrad.at[slot])

        @pl.loop(0, chips)
        def _(z):
            part_copy(slot, z).wait_send()

            @pl.when((z > chip) & has_right)
            def _():
                right_copy(slot, z).wait_send()

            @pl.when((z < chip) & has_left)
            def _():
                left_copy(slot, z).wait_send()

        @pl.when((slot > 0) & (section > 0))
        def _():
            pass_copy(slot).wait_send()
            acc_copy(slot).wait_send()


def solution(mesh):
    n_sections, n_tp = mesh.shape["section"], mesh.shape["tp"]

    def body(grad_in, fresh, acc_in, queries, keys, values, wq, wk, wv, wo):
        slots = queries.shape[1]
        rows, width = grad_in.shape[1:]
        columns = queries.shape[3]
        chips = n_tp // 2
        vmem = pl.BlockSpec(memory_space=pltpu.VMEM)
        hbm = pl.BlockSpec(memory_space=pl.ANY)
        block = (slots, chips, rows, width)
        scratch = [
            pltpu.VMEM(wq.shape[1:], BF16),
            pltpu.VMEM(wk.shape[1:], BF16),
            pltpu.VMEM(wv.shape[1:], BF16),
            pltpu.VMEM(wo.shape[1:], BF16),
            pltpu.VMEM((slots, rows, width), BF16),
            pltpu.VMEM((2 * slots, n_tp, rows, width), BF16),
            pltpu.VMEM((slots, rows, columns), BF16),
            pltpu.VMEM((rows, columns), BF16),
            pltpu.VMEM((rows, columns), BF16),
            pltpu.VMEM((rows, columns), F32),
            pltpu.VMEM((slots, rows, width), BF16),
            pltpu.VMEM((chips, rows, width), F32),
        ]
        scratch += [pltpu.VMEM(block, BF16)] * 6
        scratch += [pltpu.VMEM((slots, rows, width), BF16)] * 2
        dma = pltpu.SemaphoreType.DMA
        scratch += [
            dma((5,)),
            dma((2 * slots, chips, CHUNKS, 3)),
            dma((2 * slots, n_tp, CHUNKS)),
            dma((2, slots, chips)),
            dma((2, slots, chips)),
            dma((2, slots, chips)),
            dma((2, slots)),
            dma((2, slots)),
        ]
        return pl.pallas_call(
            functools.partial(kernel, n_sections, n_tp, slots),
            out_shape=(
                jax.ShapeDtypeStruct(grad_in.shape, BF16),
                jax.ShapeDtypeStruct(acc_in.shape, F32),
            ),
            in_specs=[hbm, hbm, vmem, vmem, vmem, vmem, hbm, hbm, hbm, hbm],
            out_specs=(vmem, vmem),
            scratch_shapes=scratch,
            compiler_params=pltpu.CompilerParams(
                collective_id=0, has_side_effects=True, vmem_limit_bytes=60 * 1024 * 1024
            ),
        )(grad_in, fresh, acc_in, queries, keys, values, wq, wk, wv, wo)

    in_specs = (
        P("section", None, "tp"),
        P(None, None, "tp"),
        P("section", None, "tp"),
        P("section", None, None, "tp"),
        P("section", None, None, "tp"),
        P("section", None, None, "tp"),
        P("section", "tp", None),
        P("section", None, "tp"),
        P("section", None, "tp"),
        P("section", "tp", None),
    )
    out_specs = (P("section", None, "tp"), P("section", None, "tp"))
    return jax.shard_map(body, mesh=mesh, in_specs=in_specs, out_specs=out_specs, check_vma=False)
```

```python
import functools

import jax
import jax.numpy as jnp
from jax import lax
from jax.experimental import pallas as pl
from jax.experimental.pallas import tpu as pltpu
from jax.sharding import PartitionSpec as P

HEAD_DIM = 64
LANES = 128
CHUNKS = 2
MESH = pl.DeviceIdType.MESH
F32, BF16 = jnp.float32, jnp.bfloat16


def nt(left, right):
    return lax.dot_general(left, right, (((1,), (1,)), ((), ())), preferred_element_type=F32)


def tn(left, right):
    return lax.dot_general(left, right, (((0,), (0,)), ((), ())), preferred_element_type=F32)


def nn(left, right):
    return lax.dot_general(left, right, (((1,), (0,)), ((), ())), preferred_element_type=F32)


def kernel(
    n_sections, n_tp, slots,
    grad_in, fresh, acc_in, queries, keys, values, wq_hbm, wk_hbm, wv_hbm, wo_hbm,
    grad_out, acc_out,
    wq, wk, wv, wo, gbuf, gathered, qgrad, kgrad, vgrad, total, passed_buf,
    own_term, part_out, part_in, right_out, right_in, left_out, left_in, acc_send, acc_recv,
    load_sem, ag_send, ag_recv, part_sem, right_sem, left_sem, pass_sem, acc_sem,
):
    section = lax.axis_index("section")
    me = lax.axis_index("tp")
    chips = n_tp // 2
    chip, core = me // 2, me % 2
    other = 1 - core
    partner = chip * 2 + other
    rows, width = grad_in.shape[1], grad_in.shape[2]
    columns = queries.shape[3]
    chunks, piece = gbuf.shape[1], gbuf.shape[3]
    has_left, has_right = chip > 0, chip < chips - 1
    top = section == n_sections - 1

    def part_of(c):
        return pl.ds(c * piece, piece)

    def load(source, target, n):
        return pltpu.make_async_copy(source, target, load_sem.at[n])

    loads = [
        load(wo_hbm.at[0], wo, 0),
        load(wk_hbm.at[0], wk, 1),
        load(wv_hbm.at[0], wv, 2),
        load(wq_hbm.at[0], wq, 3),
    ]
    first_grads = [load(grad_in.at[0, :, part_of(c)], gbuf.at[0, c], 4 + c) for c in range(chunks)]
    for one in first_grads + loads:
        one.start()

    barrier = pltpu.get_barrier_semaphore()

    def greet(condition, device):
        @pl.when(condition)
        def _():
            pl.semaphore_signal(barrier, inc=1, device_id=device, device_id_type=MESH)

    neighbours = [
        (core >= 0, {"tp": partner}),
        (has_left, {"tp": me - 2}),
        (has_right, {"tp": me + 2}),
        (section > 0, {"section": section - 1}),
        (section < n_sections - 1, {"section": section + 1}),
    ]
    for condition, device in neighbours:
        greet(condition, device)
    pl.semaphore_wait(barrier, sum(jnp.where(condition, 1, 0) for condition, _ in neighbours))

    def block_copy(source, i, block, c, way, device):
        return pltpu.make_async_remote_copy(
            src_ref=source.at[c],
            dst_ref=gathered.at[i, block, c],
            send_sem=ag_send.at[i, block // 2, c, way],
            recv_sem=ag_recv.at[i, block, c],
            device_id={"tp": device},
            device_id_type=MESH,
        )

    def start_gather(i, source, c):
        @pl.when(has_right)
        def _():
            block_copy(source, i, me, c, 0, me + 2).start()

        @pl.when(has_left)
        def _():
            block_copy(source, i, me, c, 1, me - 2).start()

        block_copy(source, i, me, c, 2, partner).start()

    def relay(i, h):
        for c in range(chunks):
            @pl.when((h > 0) & (chip - h >= 0))
            def _():
                block = (chip - h) * 2 + core
                held = gathered.at[i, block]
                block_copy(held, i, block, c, 2, partner).wait_recv()

                @pl.when(has_right)
                def _():
                    block_copy(held, i, block, c, 0, me + 2).start()

                block_copy(held, i, block, c, 2, partner).start()

            @pl.when((h > 0) & (chip + h < chips))
            def _():
                block = (chip + h) * 2 + core
                held = gathered.at[i, block]
                block_copy(held, i, block, c, 2, partner).wait_recv()

                @pl.when(has_left)
                def _():
                    block_copy(held, i, block, c, 1, me - 2).start()

                block_copy(held, i, block, c, 2, partner).start()

    def product(source, weight, block):
        result = 0.0
        for c in range(chunks):
            at = pl.ds(pl.multiple_of(block * width + c * piece, piece), piece)
            result = result + nt(source[c], weight[:, at])
        return result

    def add_block(i, weight, block):
        total[...] += product(gathered.at[i, block], weight, block)

    def take(i, weight, h):
        for condition, chip_of in (((h > 0) & (chip - h >= 0), chip - h), ((h > 0) & (chip + h < chips), chip + h)):
            @pl.when(condition)
            def _():
                add_block(i, weight, chip_of * 2 + core)

    def take_partner(i, weight, h):
        for condition, chip_of in (((h >= 0) & (chip - h >= 0), chip - h), ((h > 0) & (chip + h < chips), chip + h)):
            @pl.when(condition)
            def _():
                block = chip_of * 2 + other
                for c in range(chunks):
                    block_copy(gathered.at[i, block], i, block, c, 2, partner).wait_recv()
                add_block(i, weight, block)

    def own_block(source, weight):
        total[...] = product(source, weight, me)

    def wait_gather_sends(i, source):
        @pl.loop(0, chips)
        def _(o):
            block = o * 2 + core
            for c in range(chunks):
                @pl.when(has_right & (o <= chip))
                def _():
                    block_copy(source, i, block, c, 0, me + 2).wait_send()

                @pl.when(has_left & (o >= chip))
                def _():
                    block_copy(source, i, block, c, 1, me - 2).wait_send()

                block_copy(source, i, block, c, 2, partner).wait_send()

    def attention_grads(slot, then):
        per_chunk = piece // LANES
        lane = lax.broadcasted_iota(jnp.int32, (1, LANES), 1)
        masks = [
            ((lane >= n * HEAD_DIM) & (lane < (n + 1) * HEAD_DIM)).astype(F32).astype(BF16)
            for n in range(LANES // HEAD_DIM)
        ]
        for pair in range(columns // LANES):
            at = pl.ds(pair * LANES, LANES)
            query, key, value = queries[0, slot, :, at], keys[0, slot, :, at], values[0, slot, :, at]
            upstream = total[:, at].astype(BF16)
            dq, dk, dv = 0.0, 0.0, 0.0
            for mask in masks:
                key_h = key * mask
                scores = nt(query, key_h)
                prob_grad = nt(upstream, value * mask)
                shifted = jnp.exp(scores - jnp.max(scores, axis=1, keepdims=True))
                attention = shifted / jnp.sum(shifted, axis=1, keepdims=True)
                weights = attention.astype(BF16)
                delta = jnp.sum(weights.astype(F32) * prob_grad, axis=1, keepdims=True)
                score_grad = (attention * (prob_grad - delta)).astype(BF16)
                dq = dq + nn(score_grad, key_h)
                dk = dk + tn(score_grad, query * mask)
                dv = dv + tn(weights, upstream * mask)
            c, place = divmod(pair, per_chunk)
            qgrad[slot, c, :, pl.ds(place * LANES, LANES)] = dq.astype(BF16)
            kgrad[:, at] = dk.astype(BF16)
            vgrad[:, at] = dv.astype(BF16)
            if place == per_chunk - 1:
                then(c)

    def part_copy(slot, z):
        return pltpu.make_async_remote_copy(
            src_ref=part_out.at[slot, z], dst_ref=part_in.at[slot, z],
            send_sem=part_sem.at[0, slot, z], recv_sem=part_sem.at[1, slot, z],
            device_id={"tp": partner}, device_id_type=MESH,
        )

    def right_copy(slot, z):
        return pltpu.make_async_remote_copy(
            src_ref=right_out.at[slot, z], dst_ref=right_in.at[slot, z],
            send_sem=right_sem.at[0, slot, z], recv_sem=right_sem.at[1, slot, z],
            device_id={"tp": me + 2}, device_id_type=MESH,
        )

    def left_copy(slot, z):
        return pltpu.make_async_remote_copy(
            src_ref=left_out.at[slot, z], dst_ref=left_in.at[slot, z],
            send_sem=left_sem.at[0, slot, z], recv_sem=left_sem.at[1, slot, z],
            device_id={"tp": me - 2}, device_id_type=MESH,
        )

    def term_block(z, core_of):
        at = pl.ds(pl.multiple_of((z * 2 + core_of) * width, LANES), width)
        return nt(kgrad[...], wk[at, :]) + nt(vgrad[...], wv[at, :])

    def make_terms(slot):
        @pl.loop(0, chips)
        def _(k):
            z = (2 * chips - 1 - chip + k) % chips
            part_out[slot, z] = term_block(z, other).astype(BF16)
            part_copy(slot, z).start()

        @pl.loop(0, chips)
        def _(z):
            own_term[z] = term_block(z, core)

    def sum_step(slot, h):
        @pl.when(chip == h)
        def _():
            @pl.loop(0, chips)
            def _(j):
                z = chips - 1 - j

                @pl.when(z > chip)
                def _():
                    part_copy(slot, z).wait_recv()

                    @pl.when(has_left)
                    def _():
                        right_copy(slot, z).wait_recv()
                        own_term[z] += right_in[slot, z].astype(F32)

                    right_out[slot, z] = (own_term[z] + part_in[slot, z].astype(F32)).astype(BF16)
                    right_copy(slot, z).start()

        @pl.when(chips - 1 - chip == h)
        def _():
            @pl.loop(0, chips)
            def _(z):
                @pl.when(z < chip)
                def _():
                    part_copy(slot, z).wait_recv()

                    @pl.when(has_right)
                    def _():
                        left_copy(slot, z).wait_recv()
                        own_term[z] += left_in[slot, z].astype(F32)

                    left_out[slot, z] = (own_term[z] + part_in[slot, z].astype(F32)).astype(BF16)
                    left_copy(slot, z).start()

    def finish_sum(slot):
        part_copy(slot, chip).wait_recv()
        own_term[chip] += part_in[slot, chip].astype(F32)

        @pl.when(has_left)
        def _():
            right_copy(slot, chip).wait_recv()
            own_term[chip] += right_in[slot, chip].astype(F32)

        @pl.when(has_right)
        def _():
            left_copy(slot, chip).wait_recv()
            own_term[chip] += left_in[slot, chip].astype(F32)

        @pl.when(slot == 0)
        def _():
            own_term[chip] += acc_in[0]

        @pl.when((slot > 0) & (section < n_sections - 1))
        def _():
            acc_copy(slot).wait_recv()
            own_term[chip] += acc_recv[slot].astype(F32)

        @pl.when(slot == slots - 1)
        def _():
            acc_out[0] = own_term[chip]

        @pl.when((slot < slots - 1) & (section > 0))
        def _():
            acc_send[slot] = own_term[chip].astype(BF16)
            acc_copy(slot + 1).start()

    def acc_copy(slot):
        return pltpu.make_async_remote_copy(
            src_ref=acc_send.at[slot - 1], dst_ref=acc_recv.at[slot],
            send_sem=acc_sem.at[0, slot], recv_sem=acc_sem.at[1, slot],
            device_id={"section": section - 1}, device_id_type=MESH,
        )

    def pass_copy(slot, c):
        return pltpu.make_async_remote_copy(
            src_ref=passed_buf.at[slot - 1, c], dst_ref=gbuf.at[slot, c],
            send_sem=pass_sem.at[0, slot, c], recv_sem=pass_sem.at[1, slot, c],
            device_id={"section": section - 1}, device_id_type=MESH,
        )

    def fresh_copy(slot, c):
        return load(fresh.at[slot - 1, :, part_of(c)], gbuf.at[slot, c], 4 + c)

    @pl.loop(0, slots)
    def _(slot):
        first = slot * 2
        second = first + 1
        for c in range(chunks):
            @pl.when(slot == 0)
            def _():
                first_grads[c].wait()

            @pl.when((slot > 0) & top)
            def _():
                fresh_copy(slot, c).start()
                fresh_copy(slot, c).wait()

            @pl.when((slot > 0) & (section < n_sections - 1))
            def _():
                pass_copy(slot, c).wait_recv()

            start_gather(first, gbuf.at[slot], c)

        @pl.when(slot == 0)
        def _():
            loads[0].wait()

        own_block(gbuf.at[slot], wo)

        @pl.when(slot > 0)
        def _():
            finish_sum(slot - 1)

        @pl.loop(1, chips)
        def _(h):
            relay(first, h)
            take(first, wo, h)
            take_partner(first, wo, h - 1)

        take_partner(first, wo, chips - 1)
        attention_grads(slot, lambda c: start_gather(second, qgrad.at[slot], c))

        @pl.when(slot == 0)
        def _():
            loads[1].wait()
            loads[2].wait()

        make_terms(slot)

        @pl.when(slot == 0)
        def _():
            loads[3].wait()

        own_block(qgrad.at[slot], wq)

        @pl.loop(0, chips)
        def _(h):
            relay(second, h)
            sum_step(slot, h)
            take(second, wq, h)
            take_partner(second, wq, h - 1)

        take_partner(second, wq, chips - 1)
        for c in range(chunks):
            result = (gbuf[slot, c].astype(F32) + total[:, part_of(c)]).astype(BF16)

            @pl.when(slot == slots - 1)
            def _():
                grad_out[0, :, part_of(c)] = result

            @pl.when((slot < slots - 1) & (section > 0))
            def _():
                passed_buf[slot, c] = result
                pass_copy(slot + 1, c).start()

    finish_sum(slots - 1)

    @pl.loop(0, slots)
    def _(slot):
        wait_gather_sends(slot * 2, gbuf.at[slot])
        wait_gather_sends(slot * 2 + 1, qgrad.at[slot])

        @pl.loop(0, chips)
        def _(z):
            part_copy(slot, z).wait_send()

            @pl.when((z > chip) & has_right)
            def _():
                right_copy(slot, z).wait_send()

            @pl.when((z < chip) & has_left)
            def _():
                left_copy(slot, z).wait_send()

        @pl.when((slot > 0) & (section > 0))
        def _():
            for c in range(chunks):
                pass_copy(slot, c).wait_send()
            acc_copy(slot).wait_send()


def solution(mesh):
    n_sections, n_tp = mesh.shape["section"], mesh.shape["tp"]

    def body(grad_in, fresh, acc_in, queries, keys, values, wq, wk, wv, wo):
        slots = queries.shape[1]
        rows, width = grad_in.shape[1:]
        columns = queries.shape[3]
        chips = n_tp // 2
        chunks = max(1, min(CHUNKS, width // LANES))
        pieces = (chunks, rows, width // chunks)
        vmem = pl.BlockSpec(memory_space=pltpu.VMEM)
        hbm = pl.BlockSpec(memory_space=pl.ANY)
        block = (slots, chips, rows, width)
        scratch = [
            pltpu.VMEM(wq.shape[1:], BF16),
            pltpu.VMEM(wk.shape[1:], BF16),
            pltpu.VMEM(wv.shape[1:], BF16),
            pltpu.VMEM(wo.shape[1:], BF16),
            pltpu.VMEM((slots, *pieces), BF16),
            pltpu.VMEM((2 * slots, n_tp, *pieces), BF16),
            pltpu.VMEM((slots, *pieces), BF16),
            pltpu.VMEM((rows, columns), BF16),
            pltpu.VMEM((rows, columns), BF16),
            pltpu.VMEM((rows, columns), F32),
            pltpu.VMEM((slots, *pieces), BF16),
            pltpu.VMEM((chips, rows, width), F32),
        ]
        scratch += [pltpu.VMEM(block, BF16)] * 6
        scratch += [pltpu.VMEM((slots, rows, width), BF16)] * 2
        dma = pltpu.SemaphoreType.DMA
        scratch += [
            dma((4 + chunks,)),
            dma((2 * slots, chips, chunks, 3)),
            dma((2 * slots, n_tp, chunks)),
            dma((2, slots, chips)),
            dma((2, slots, chips)),
            dma((2, slots, chips)),
            dma((2, slots, chunks)),
            dma((2, slots)),
        ]
        return pl.pallas_call(
            functools.partial(kernel, n_sections, n_tp, slots),
            out_shape=(
                jax.ShapeDtypeStruct(grad_in.shape, BF16),
                jax.ShapeDtypeStruct(acc_in.shape, F32),
            ),
            in_specs=[hbm, hbm, vmem, vmem, vmem, vmem, hbm, hbm, hbm, hbm],
            out_specs=(vmem, vmem),
            scratch_shapes=scratch,
            compiler_params=pltpu.CompilerParams(
                collective_id=0, has_side_effects=True, vmem_limit_bytes=60 * 1024 * 1024
            ),
        )(grad_in, fresh, acc_in, queries, keys, values, wq, wk, wv, wo)

    in_specs = (
        P("section", None, "tp"),
        P(None, None, "tp"),
        P("section", None, "tp"),
        P("section", None, None, "tp"),
        P("section", None, None, "tp"),
        P("section", None, None, "tp"),
        P("section", "tp", None),
        P("section", None, "tp"),
        P("section", None, "tp"),
        P("section", "tp", None),
    )
    out_specs = (P("section", None, "tp"), P("section", None, "tp"))
    return jax.shard_map(body, mesh=mesh, in_specs=in_specs, out_specs=out_specs, check_vma=False)
```
